32 devices in a mesh: data: 4 (over y, z), cp: 8 (over x, core).
Axes of the slice: x: 4, y: 2, z: 2, core: 2. Of those that a mesh axis runs over, the one named last changes fastest.
The devices are a block of a 4x4x8 slice.
Arguments:
- q: bfloat16 [32768, 4, 128], P(('data', 'cp')), parts along dimension 0
- k: bfloat16 [32768, 4, 128], P(('data', 'cp')), parts along dimension 0
- v: bfloat16 [32768, 4, 128], P(('data', 'cp')), parts along dimension 0
- o: bfloat16 [32768, 4, 128], P(('data', 'cp')), parts along dimension 0
- dout: bfloat16 [32768, 4, 128], P(('data', 'cp')), parts along dimension 0
- lse: float32 [4, 32768], P(None, ('data', 'cp')), parts along dimension 1
Outputs:
- output 1: bfloat16 [32768, 4, 128], P(('data', 'cp')), parts along dimension 0
- output 2: bfloat16 [32768, 4, 128], P(('data', 'cp')), parts along dimension 0
- output 3: bfloat16 [32768, 4, 128], P(('data', 'cp')), parts along dimension 0
There are 4 independent parts. The reference program is written for one: setup_inputs(seed, part) draws one part's arguments, and reference() takes and returns one part's arrays. A program takes and returns all parts, laid end to end along the dimension named above; each array names one.
All inputs are finite; a program needn't handle non-finite values.
Results may differ from the reference program's by a relative error of at most 0.001.
Values are sent between devices in bfloat16 or wider.
A program may use at most 768 MiB of HBM per device.

```python
import math
import jax
import jax.numpy as jnp
from jax import lax

C = 1024
CP = 8
HEADS = 4
HEAD = 128
QB = 128

T = C * CP
SCALE = 1.0 / math.sqrt(HEAD)


def positions():
    r = jnp.arange(T, dtype=jnp.int32)
    return (r % C) * CP + r // C


def _head_forward(q, k, v, pos):
    def blk(b):
        qb = lax.dynamic_slice_in_dim(q, b * QB, QB)
        pb = lax.dynamic_slice_in_dim(pos, b * QB, QB)
        s = jnp.dot(qb, k.T, preferred_element_type=jnp.float32) * SCALE
        s = jnp.where(pos[None, :] <= pb[:, None], s, -jnp.inf)
        mx = jnp.max(s, axis=1, keepdims=True)
        e = jnp.exp(s - mx)
        l = jnp.sum(e, axis=1, keepdims=True)
        o = jnp.dot((e / l).astype(jnp.bfloat16), v, preferred_element_type=jnp.float32)
        return o.astype(jnp.bfloat16), (mx + jnp.log(l))[:, 0]
    o, lse = lax.map(blk, jnp.arange(T // QB))
    return o.reshape(T, HEAD), lse.reshape(T)


def _forward(q, k, v):
    pos = positions()
    o, lse = lax.map(lambda a: _head_forward(a[0], a[1], a[2], pos),
                     (q.transpose(1, 0, 2), k.transpose(1, 0, 2), v.transpose(1, 0, 2)))
    return o.transpose(1, 0, 2), lse


def setup_inputs(seed: int = 0, part: int = 0) -> dict:
    key = jax.random.fold_in(jax.random.PRNGKey(seed), part)
    kq, kk, km, kv, kd = jax.random.split(key, 5)
    shape = (T, HEADS, HEAD)
    q = jax.random.normal(kq, shape, jnp.float32).astype(jnp.bfloat16)
    k = jax.random.normal(kk, shape, jnp.float32).astype(jnp.bfloat16)
    mu = jax.random.normal(km, (1, HEADS, HEAD), jnp.float32)
    v = (0.8 * mu + 0.6 * jax.random.normal(kv, shape, jnp.float32)).astype(jnp.bfloat16)
    o, lse = _forward(q, k, v)
    dout = (0.8 * o.astype(jnp.float32) + 0.6 * jax.random.normal(kd, shape, jnp.float32)).astype(jnp.bfloat16)
    return {'q': q, 'k': k, 'v': v, 'o': o, 'dout': dout, 'lse': lse}


def reference(q, k, v, o, dout, lse):
    pos = positions()
    dd = jnp.sum(dout.astype(jnp.float32) * o.astype(jnp.float32), axis=-1)

    def head(a):
        qh, kh, vh, doh, lh, dh = a

        def step(carry, b):
            dk, dv = carry
            qb = lax.dynamic_slice_in_dim(qh, b * QB, QB)
            dob = lax.dynamic_slice_in_dim(doh, b * QB, QB)
            lb = lax.dynamic_slice_in_dim(lh, b * QB, QB)
            db = lax.dynamic_slice_in_dim(dh, b * QB, QB)
            pb = lax.dynamic_slice_in_dim(pos, b * QB, QB)
            s = jnp.dot(qb, kh.T, preferred_element_type=jnp.float32) * SCALE
            mask = pos[None, :] <= pb[:, None]
            p = jnp.where(mask, jnp.exp(s - lb[:, None]), 0.0)
            dv = dv + jnp.dot(p.astype(jnp.bfloat16).T, dob, preferred_element_type=jnp.float32)
            dp = jnp.dot(dob, vh.T, preferred_element_type=jnp.float32)
            ds = (p * (dp - db[:, None])).astype(jnp.bfloat16)
            dqb = jnp.dot(ds, kh, preferred_element_type=jnp.float32) * SCALE
            dk = dk + jnp.dot(ds.T, qb, preferred_element_type=jnp.float32) * SCALE
            return (dk, dv), dqb

        z = jnp.zeros((T, HEAD), jnp.float32)
        (dk, dv), dq = lax.scan(step, (z, z), jnp.arange(T // QB))
        return dq.reshape(T, HEAD), dk, dv

    dq, dk, dv = lax.map(head, (q.transpose(1, 0, 2), k.transpose(1, 0, 2), v.transpose(1, 0, 2),
                                dout.transpose(1, 0, 2), lse, dd.T))
    return (dq.transpose(1, 0, 2).astype(jnp.bfloat16),
            dk.transpose(1, 0, 2).astype(jnp.bfloat16),
            dv.transpose(1, 0, 2).astype(jnp.bfloat16))
```

```python
import functools

import jax
import jax.numpy as jnp
from jax import lax
from jax.experimental import pallas as pl
from jax.experimental.pallas import tpu as pltpu
from jax.sharding import PartitionSpec as P

TB = 64
LOG2E = 1.4426950408889634
MESH = pl.DeviceIdType.MESH
NN = (((1,), (0,)), ((), ()))
NT = (((1,), (1,)), ((), ()))
TN = (((0,), (0,)), ((), ()))


def _dot(a, b, dims):
    return lax.dot_general(a, b, dims, preferred_element_type=jnp.float32)


def _kernel(n, scale, q_ref, k_ref, v_ref, do_ref, ld_ref, oq_ref, ok_ref, ov_ref,
            qx, dox, kx, vx, ldx, lseb, db, rel, dq, dqr, dk, dv, dqo, dko, dvo,
            s_in, r_in, s_ld, r_ld, s_fw, r_fw, s_dq, r_dq, s_out, r_out):
    f32, bf16 = jnp.float32, jnp.bfloat16
    me = lax.axis_index('cp')
    x, c = lax.div(me, 2), lax.rem(me, 2)
    sib = x * 2 + (1 - c)
    ni = kx.shape[0]
    blk = n * TB
    d = q_ref.shape[-1]
    split = ni - 2

    def own(core, i):
        return 2 * i + lax.rem(core + i, 2)

    def rows(b):
        return pl.ds(pl.multiple_of(b * TB, TB), TB)

    def copy(src, dst, s, r, dev):
        return pltpu.make_async_remote_copy(src_ref=src, dst_ref=dst, send_sem=s, recv_sem=r,
                                            device_id={'cp': dev}, device_id_type=MESH)

    bar = pltpu.get_barrier_semaphore()
    for t in range(1, n):
        pl.semaphore_signal(bar, 1, device_id={'cp': lax.rem(me + t, n)}, device_id_type=MESH)
    pl.semaphore_wait(bar, n - 1)

    def send_ld(t, _):
        to = lax.rem(me + t, n)
        copy(ld_ref.at[lax.div(to, 2)], ldx.at[me], s_ld, r_ld, to).start()
        return 0

    lax.fori_loop(1, n, send_ld, 0)
    ins = ((q_ref, qx), (do_ref, dox), (k_ref, kx), (v_ref, vx))

    def send_block(i, _):
        def to_dev(t, _):
            to = lax.rem(me + t, n)
            h, b = lax.div(to, 2), own(lax.rem(to, 2), i)
            for a, (src, dst) in enumerate(ins):
                copy(src.at[h, rows(b)], dst.at[b if a < 2 else i, me], s_in.at[a], r_in.at[i, a], to).start()
            return 0
        lax.fori_loop(1, n, to_dev, 0)
        return 0

    lax.fori_loop(0, ni, send_block, 0)

    def keep(i, _):
        b = own(c, i)
        qx[b, me] = q_ref[x, rows(b)]
        dox[b, me] = do_ref[x, rows(b)]
        kx[i, me] = k_ref[x, rows(b)]
        vx[i, me] = v_ref[x, rows(b)]
        return 0

    lax.fori_loop(0, ni, keep, 0)
    ldx[me] = ld_ref[x]

    def zero(i, _):
        dk[i] = jnp.zeros((blk, d), f32)
        dv[i] = jnp.zeros((blk, d), f32)
        dq[2 * i] = jnp.zeros((blk, d), f32)
        dq[2 * i + 1] = jnp.zeros((blk, d), f32)
        return 0

    lax.fori_loop(0, ni, zero, 0)

    def rel_rows(j, _):
        tt = lax.broadcasted_iota(jnp.int32, (TB, 2 * blk), 0)
        ql = lax.broadcasted_iota(jnp.int32, (TB, 2 * blk), 1)
        l2 = lax.rem(ql, blk)
        qpos = (ql - l2) + lax.rem(l2, TB) * n + lax.div(l2, TB)
        rel[rows(j)] = tt * n + j - qpos
        return 0

    lax.fori_loop(0, n, rel_rows, 0)

    def wait_in(i):
        for a in range(4):
            part = kx.at[0, pl.ds(0, n - 1)]
            copy(part, part, s_in.at[a], r_in.at[i, a], sib).wait_recv()

    def forward(i):
        b = own(c, i)
        copy(qx.at[b], qx.at[b], s_fw.at[0], r_fw.at[i, 0], sib).start()
        copy(dox.at[b], dox.at[b], s_fw.at[1], r_fw.at[i, 1], sib).start()

    def wait_forward(i):
        for a in range(2):
            copy(kx.at[0], kx.at[0], s_fw.at[a], r_fw.at[i, a], sib).wait_recv()

    wait_in(0)
    forward(0)
    part = ldx.at[pl.ds(0, n - 1)]
    copy(part, part, s_ld, r_ld, sib).wait_recv()
    low = lax.broadcasted_iota(jnp.int32, (ni, 2 * TB), 1) < TB
    for m in range(n // 2):
        for w, dst, f in ((0, lseb, LOG2E), (1, db, 1.0)):
            a, b = ldx[2 * m, w] * f, ldx[2 * m + 1, w] * f
            dst[:, pl.ds(m * 2 * TB, 2 * TB)] = jnp.where(low, a, pltpu.roll(b, TB, 1))
            dst[:, pl.ds(blk + m * 2 * TB, 2 * TB)] = jnp.where(low, pltpu.roll(a, TB, 1), b)

    def tile(i, p, masked):
        q = qx[pl.ds(2 * p, 2)].reshape(2 * blk, d)
        do = dox[pl.ds(2 * p, 2)].reshape(2 * blk, d)
        k = kx[i].reshape(blk, d)
        v = vx[i].reshape(blk, d)
        s = _dot(k, q, NT)
        pr = jnp.exp2(s * (scale * LOG2E) - lseb[pl.ds(p, 1), :])
        if masked:
            pr = jnp.where(rel[...] <= -blk * lax.rem(c + i, 2), pr, 0.0)
        dv[i] += _dot(pr.astype(bf16), do, NN)
        dp = _dot(v, do, NT)
        ds = (pr * (dp - db[pl.ds(p, 1), :])).astype(bf16)
        dk[i] += _dot(ds, q, NN)
        dq[pl.ds(2 * p, 2)] += _dot(ds, k, TN).reshape(2, blk, d)

    def either(i, p):
        @pl.when(i < p)
        def _():
            tile(i, p, False)

        @pl.when(i == p)
        def _():
            tile(i, p, True)

    def dq_swap(p):
        copy(dq.at[own(1 - c, p)], dqr.at[p], s_dq, r_dq.at[p], sib).start()

    def dq_join(p):
        copy(dqr.at[0], dqr.at[0], s_dq, r_dq.at[p], sib).wait_recv()
        g = ((dq[own(c, p)] + dqr[p]) * scale).astype(bf16)
        dqo[p] = g.reshape(n, TB, d)

    def send_out(src, dst, a, i):
        b = own(c, i)

        def to_dev(t, _):
            to = lax.rem(me + t, n)
            copy(src.at[i, to], dst.at[x, rows(b)], s_out.at[a], r_out.at[a], to).start()
            return 0

        lax.fori_loop(1, n, to_dev, 0)
        dst[x, rows(b)] = src[i, me]

    def dq_send(p):
        send_out(dqo, oq_ref, 0, p)

    def kv_round(i):
        dko[i] = (dk[i] * scale).astype(bf16).reshape(n, TB, d)
        dvo[i] = dv[i].astype(bf16).reshape(n, TB, d)

    def kv_send(i):
        send_out(dko, ok_ref, 1, i)
        send_out(dvo, ov_ref, 2, i)

    def row(p, _):
        wait_forward(p)

        def step(i, _):
            @pl.when(i == p)
            def _():
                wait_in(p + 1)
                forward(p + 1)

            either(i, p)

            @pl.when((i == 0) & (p >= 1))
            def _():
                dq_swap(p - 1)

            @pl.when((i == 0) & (p >= 2))
            def _():
                dq_send(p - 2)
            return 0

        lax.fori_loop(0, p + 1, step, 0)

        @pl.when(p >= 1)
        def _():
            dq_join(p - 1)
        return 0

    lax.fori_loop(0, split, row, 0)

    wait_forward(split)
    wait_in(split + 1)
    forward(split + 1)

    def column(i, _):
        @pl.when(i <= split)
        def _():
            either(i, split)

        @pl.when(i == 0)
        def _():
            dq_swap(split - 1)
            dq_send(split - 2)
            wait_forward(split + 1)

        @pl.when(i >= 1)
        def _():
            kv_send(i - 1)

        @pl.when(i == 1)
        def _():
            dq_send(split - 1)

        either(i, split + 1)

        @pl.when(i == 0)
        def _():
            dq_join(split - 1)

        @pl.when(i == split)
        def _():
            dq_swap(split)

        kv_round(i)
        return 0

    lax.fori_loop(0, ni, column, 0)
    dq_swap(split + 1)
    dq_join(split)
    kv_send(ni - 1)
    dq_join(split + 1)
    dq_send(split)
    dq_send(split + 1)

    part = kx.at[pl.ds(0, n - 1)]
    for a in range(3):
        copy(part, part, s_out.at[a], r_out.at[a], sib).wait()
    for a in range(4):
        copy(part, part, s_in.at[a], r_out.at[0], sib).wait_send()
    for a in range(2):
        copy(kx, kx, s_fw.at[a], r_out.at[0], sib).wait_send()
    copy(dqr, dqr, s_dq, r_out.at[0], sib).wait_send()
    part = ldx.at[pl.ds(0, n - 1)]
    copy(part, part, s_ld, r_out.at[0], sib).wait_send()


def solution(mesh):
    n = mesh.shape['cp']
    rows = P(('data', 'cp'))
    cols = P(None, ('data', 'cp'))

    def local(q, k, v, o, dout, lse):
        c, h, d = q.shape
        assert 2 * h == n and d == 2 * TB and c % (2 * TB) == 0 and n * TB % 128 == 0
        ni = c // (2 * TB)
        blk = n * TB
        f32, bf16 = jnp.float32, jnp.bfloat16
        dd = jnp.einsum('qhd,qhd->hq', dout, o, preferred_element_type=f32)
        ld = jnp.stack([lse, dd], axis=1).reshape(h, 2, ni, 2 * TB)
        heads = [a.transpose(1, 0, 2) for a in (q, k, v, dout)]
        vm = pl.BlockSpec(memory_space=pltpu.VMEM)
        dma = pltpu.SemaphoreType.DMA
        outs = pl.pallas_call(
            functools.partial(_kernel, n, d ** -0.5),
            out_shape=[jax.ShapeDtypeStruct((h, c, d), bf16)] * 3,
            in_specs=[vm] * 5,
            out_specs=[vm] * 3,
            scratch_shapes=[
                pltpu.VMEM((2 * ni, n, TB, d), bf16),
                pltpu.VMEM((2 * ni, n, TB, d), bf16),
                pltpu.VMEM((ni, n, TB, d), bf16),
                pltpu.VMEM((ni, n, TB, d), bf16),
                pltpu.VMEM((n, 2, ni, 2 * TB), f32),
                pltpu.VMEM((ni, 2 * blk), f32),
                pltpu.VMEM((ni, 2 * blk), f32),
                pltpu.VMEM((blk, 2 * blk), jnp.int32),
                pltpu.VMEM((2 * ni, blk, d), f32),
                pltpu.VMEM((ni, blk, d), f32),
                pltpu.VMEM((ni, blk, d), f32),
                pltpu.VMEM((ni, blk, d), f32),
                pltpu.VMEM((ni, n, TB, d), bf16),
                pltpu.VMEM((ni, n, TB, d), bf16),
                pltpu.VMEM((ni, n, TB, d), bf16),
                dma((4,)), dma((ni, 4)), dma, dma, dma((2,)), dma((ni, 2)), dma, dma((ni,)), dma((3,)), dma((3,)),
            ],
            compiler_params=pltpu.CompilerParams(collective_id=0, has_side_effects=True,
                                                 vmem_limit_bytes=60 * 2 ** 20),
            name='attention_grads',
        )(heads[0], heads[1], heads[2], heads[3], ld)
        return tuple(a.transpose(1, 0, 2) for a in outs)

    return jax.shard_map(local, mesh=mesh, in_specs=(rows, rows, rows, rows, rows, cols),
                         out_specs=(rows, rows, rows), check_vma=False)
```

```python
import functools

import jax
import jax.numpy as jnp
from jax import lax
from jax.experimental import pallas as pl
from jax.experimental.pallas import tpu as pltpu
from jax.sharding import PartitionSpec as P

TB = 64
LOG2E = 1.4426950408889634
MESH = pl.DeviceIdType.MESH
NN = (((1,), (0,)), ((), ()))
NT = (((1,), (1,)), ((), ()))


def _dot(a, b, dims):
    return lax.dot_general(a, b, dims, preferred_element_type=jnp.float32)


def _kernel(n, heads, scale, q_hbm, do_hbm, k_hbm, v_hbm, lse_ref, dd_ref, gq_hbm, gk_hbm, gv_hbm,
            inb, tmp, snd, ld, qx, dox, kx, vx, kt, ldx, ldb, rel, dq, dqr, dk, dv, dqo, dko, dvo, land,
            s_load, s_in, r_in, s_fw, r_fw, s_dq, r_dq, s_out, r_out, s_own):
    f32, bf16 = jnp.float32, jnp.bfloat16
    me = lax.axis_index('cp')
    x, c = lax.div(me, 2), lax.rem(me, 2)
    sib = x * 2 + (1 - c)
    ni = kx.shape[0]
    blk = n * TB
    d = q_hbm.shape[-1]
    split = ni - 2
    pr_rows = 2 * TB
    chunk = pr_rows * heads

    def own(core, i):
        return 2 * i + lax.rem(core + i, 2)

    def rows(b):
        return pl.ds(pl.multiple_of(b * TB, TB), TB)

    def span(i, size):
        return pl.ds(pl.multiple_of(i * size, size), size)

    def copy(src, dst, s, r, dev):
        return pltpu.make_async_remote_copy(src_ref=src, dst_ref=dst, send_sem=s, recv_sem=r,
                                            device_id={'cp': dev}, device_id_type=MESH)

    srcs = (q_hbm, do_hbm, k_hbm, v_hbm)

    def load(p):
        return [pltpu.make_async_copy(src.at[span(p, chunk)], inb.at[a, p], s_load.at[a, p])
                for a, src in enumerate(srcs)]

    def start_load(p, _):
        for cp in load(p):
            cp.start()
        return 0

    lax.fori_loop(0, ni, start_load, 0)

    bar = pltpu.get_barrier_semaphore()
    for t in range(1, n):
        pl.semaphore_signal(bar, 1, device_id={'cp': lax.rem(me + t, n)}, device_id_type=MESH)
    pl.semaphore_wait(bar, n - 1)

    def widen(p):
        for cp in load(p):
            cp.wait()
        for a in range(4):
            tmp[lax.rem(p, 2), a] = inb[a, p].astype(f32)

    def arrange(p):
        for h in range(heads):
            for a in range(4):
                snd[a, h, span(p, pr_rows)] = tmp[lax.rem(p, 2), a, pl.ds(h, pr_rows, stride=heads), :].astype(bf16)
            ld[h, p, 0:1] = lse_ref[pl.ds(h, 1), span(p, pr_rows)] * LOG2E
            ld[h, p, 1:2] = dd_ref[pl.ds(h, 1), span(p, pr_rows)]

    ins = (qx, dox, kx, vx)

    def send_block(i):
        def to_dev(t, _):
            to = lax.rem(me + t, n)
            h, b = lax.div(to, 2), own(lax.rem(to, 2), i)
            copy(ld.at[h, i], ldx.at[me, i], s_in.at[4], r_in.at[i, 4], to).start()
            for a, dst in enumerate(ins):
                copy(snd.at[a, h, rows(b)], dst.at[b if a < 2 else i, me], s_in.at[a], r_in.at[i, a], to).start()
            return 0
        lax.fori_loop(1, n, to_dev, 0)

    widen(0)
    widen(1)
    arrange(0)

    def feed(i, _):
        @pl.when(i < ni - 2)
        def _():
            widen(i + 2)

        @pl.when(i < ni - 1)
        def _():
            arrange(i + 1)

        send_block(i)
        return 0

    lax.fori_loop(0, ni, feed, 0)

    def keep(i, _):
        b = own(c, i)
        qx[b, me] = snd[0, x, rows(b)]
        dox[b, me] = snd[1, x, rows(b)]
        kx[i, me] = snd[2, x, rows(b)]
        vx[i, me] = snd[3, x, rows(b)]
        return 0

    lax.fori_loop(0, ni, keep, 0)
    ldx[me] = ld[x]

    def zero(i, _):
        dk[i] = jnp.zeros((blk, d), f32)
        dv[i] = jnp.zeros((blk, d), f32)
        dq[2 * i] = jnp.zeros((d, blk), f32)
        dq[2 * i + 1] = jnp.zeros((d, blk), f32)
        return 0

    lax.fori_loop(0, ni, zero, 0)

    def rel_rows(j, _):
        tt = lax.broadcasted_iota(jnp.int32, (TB, blk), 0)
        ql = lax.broadcasted_iota(jnp.int32, (TB, blk), 1)
        rel[rows(j)] = tt * n + j - lax.rem(ql, TB) * n - lax.div(ql, TB)
        return 0

    lax.fori_loop(0, n, rel_rows, 0)

    def wait_in(i):
        for a in range(4):
            part = kx.at[0, pl.ds(0, n - 1)]
            copy(part, part, s_in.at[a], r_in.at[i, a], sib).wait_recv()
        part = ldx.at[pl.ds(0, n - 1), 0]
        copy(part, part, s_in.at[4], r_in.at[i, 4], sib).wait_recv()

    low = lax.broadcasted_iota(jnp.int32, (2, pr_rows), 1) < TB

    def forward(i):
        b = own(c, i)
        copy(qx.at[b], qx.at[b], s_fw.at[0], r_fw.at[i, 0], sib).start()
        copy(dox.at[b], dox.at[b], s_fw.at[1], r_fw.at[i, 1], sib).start()
        kt[i] = kx[i].reshape(blk, d).astype(f32).T.astype(bf16)
        for m in range(n // 2):
            a, b = ldx[2 * m, i], ldx[2 * m + 1, i]
            ldb[i, :, pl.ds(m * pr_rows, pr_rows)] = jnp.where(low, a, pltpu.roll(b, TB, 1))
            ldb[i, :, pl.ds(blk + m * pr_rows, pr_rows)] = jnp.where(low, pltpu.roll(a, TB, 1), b)

    def wait_forward(i):
        for a in range(2):
            copy(kx.at[0], kx.at[0], s_fw.at[a], r_fw.at[i, a], sib).wait_recv()

    wait_in(0)
    forward(0)

    def tile(i, p, half, nb, masked):
        b = 2 * p + half
        q = qx[pl.ds(b, nb)].reshape(nb * blk, d)
        do = dox[pl.ds(b, nb)].reshape(nb * blk, d)
        cols = span(half, blk) if nb == 1 else slice(None)
        s = _dot(kx[i].reshape(blk, d), q, NT)
        pr = jnp.exp2(s * (scale * LOG2E) - ldb[p, 0:1, cols])
        if masked:
            pr = jnp.where(rel[...] <= 0, pr, 0.0)
        dv[i] += _dot(pr.astype(bf16), do, NN)
        dp = _dot(vx[i].reshape(blk, d), do, NT)
        ds = (pr * (dp - ldb[p, 1:2, cols])).astype(bf16)
        dk[i] += _dot(ds, q, NN)
        g = _dot(kt[i], ds, NN)
        for m in range(nb):
            dq[b + m] += g[:, m * blk:(m + 1) * blk]

    def either(i, p):
        off = lax.rem(c + i, 2)

        @pl.when(i < p)
        def _():
            tile(i, p, 0, 2, False)

        @pl.when(i == p)
        def _():
            tile(i, p, off, 1, True)

        @pl.when((i == p) & (off == 0))
        def _():
            tile(i, p, 1, 1, False)

    def dq_swap(p):
        copy(dq.at[own(1 - c, p)], dqr.at[p], s_dq, r_dq.at[p], sib).start()

    def dq_join(p):
        copy(dqr.at[0], dqr.at[0], s_dq, r_dq.at[p], sib).wait_recv()
        g = (dq[own(c, p)] + dqr[p]) * scale
        dqo[p] = g.T.astype(bf16).reshape(n, TB, d)

    outs = (gq_hbm, gk_hbm, gv_hbm)

    def send_out(src, a, i):
        b = own(c, i)

        def to_dev(t, _):
            to = lax.rem(me + t, n)
            copy(src.at[i, to], land.at[a, x, rows(b)], s_out.at[a], r_out.at[a, i], to).start()
            return 0

        lax.fori_loop(1, n, to_dev, 0)
        land[a, x, rows(b)] = src[i, me]

    def dq_send(p):
        send_out(dqo, 0, p)

    def kv_round(i):
        dko[i] = (dk[i] * scale).astype(bf16).reshape(n, TB, d)
        dvo[i] = dv[i].astype(bf16).reshape(n, TB, d)

    def kv_send(i):
        send_out(dko, 1, i)
        send_out(dvo, 2, i)

    def row(p, _):
        wait_forward(p)

        def step(i, _):
            @pl.when(i == p)
            def _():
                wait_in(p + 1)
                forward(p + 1)

            either(i, p)

            @pl.when((i == 0) & (p >= 1))
            def _():
                dq_swap(p - 1)

            @pl.when((i == 0) & (p >= 2))
            def _():
                dq_send(p - 2)
            return 0

        lax.fori_loop(0, p + 1, step, 0)

        @pl.when(p >= 1)
        def _():
            dq_join(p - 1)
        return 0

    lax.fori_loop(0, split, row, 0)

    wait_forward(split)
    wait_in(split + 1)
    forward(split + 1)

    def column(i, _):
        @pl.when(i <= split)
        def _():
            either(i, split)

        @pl.when(i == 0)
        def _():
            dq_swap(split - 1)
            dq_send(split - 2)
            wait_forward(split + 1)

        @pl.when((i >= 1) & (i <= split))
        def _():
            kv_send(i - 1)

        @pl.when(i == 1)
        def _():
            dq_send(split - 1)

        either(i, split + 1)

        @pl.when(i == 0)
        def _():
            dq_join(split - 1)

        @pl.when(i == split)
        def _():
            dq_swap(split)

        @pl.when(i > split)
        def _():
            kv_send(i - 1)

        kv_round(i)
        return 0

    lax.fori_loop(0, ni, column, 0)
    dq_swap(split + 1)
    dq_join(split)
    kv_send(ni - 1)
    dq_join(split + 1)
    dq_send(split)
    dq_send(split + 1)

    def leave(a, p):
        return pltpu.make_async_copy(land.at[a, :, span(p, pr_rows)], outs[a].at[:, span(p, pr_rows)], s_own.at[a, p])

    def finish(a, p):
        part = kx.at[0, pl.ds(0, n - 1)]
        copy(part, part, s_out.at[a], r_out.at[a, p], sib).wait_recv()
        leave(a, p).start()

    def finish_q(p, _):
        finish(0, p)
        return 0

    def finish_kv(p, _):
        finish(1, p)
        finish(2, p)
        return 0

    lax.fori_loop(0, split, finish_q, 0)
    lax.fori_loop(0, ni, finish_kv, 0)
    lax.fori_loop(split, ni, finish_q, 0)

    part = kx.at[pl.ds(0, n - 1)]
    for a in range(3):
        copy(part, part, s_out.at[a], r_out.at[0, 0], sib).wait_send()
    for a in range(4):
        copy(part, part, s_in.at[a], r_out.at[0, 0], sib).wait_send()
    for a in range(2):
        copy(kx, kx, s_fw.at[a], r_out.at[0, 0], sib).wait_send()
    copy(dqr, dqr, s_dq, r_out.at[0, 0], sib).wait_send()
    part = ldx.at[pl.ds(0, n - 1)]
    copy(part, part, s_in.at[4], r_out.at[0, 0], sib).wait_send()

    def left(p, _):
        for a in range(3):
            leave(a, p).wait()
        return 0

    lax.fori_loop(0, ni, left, 0)


def _merge_kernel(heads, steps, a_hbm, b_hbm, c_hbm, x_hbm, y_hbm, z_hbm, vin, vout, tmp, s_in, s_out):
    size = vin.shape[2] // steps
    parts = [(a, r) for r in range(steps) for a in range(3)]

    def load(a, r):
        rows = pl.ds(r * size, size)
        return pltpu.make_async_copy((a_hbm, b_hbm, c_hbm)[a].at[:, rows], vin.at[a, :, rows], s_in.at[a, r])

    def store(a, r):
        rows = pl.ds(r * size * heads, size * heads)
        return pltpu.make_async_copy(vout.at[a, rows], (x_hbm, y_hbm, z_hbm)[a].at[rows], s_out.at[a, r])

    for a, r in parts:
        load(a, r).start()
    last = len(parts)
    for j in range(last + 2):
        if j < last:
            a, r = parts[j]
            load(a, r).wait()
            for h in range(heads):
                tmp[j % 2, pl.ds(h, size, stride=heads), :] = vin[a, h, pl.ds(r * size, size)].astype(jnp.float32)
        if 0 < j <= last:
            a, r = parts[j - 1]
            vout[a, pl.ds(r * size * heads, size * heads)] = tmp[(j - 1) % 2].astype(vout.dtype)
        if j > 1:
            store(*parts[j - 2]).start()
    for a, r in parts:
        store(a, r).wait()


def solution(mesh):
    n = mesh.shape['cp']
    rows = P(('data', 'cp'))
    cols = P(None, ('data', 'cp'))

    def local(q, k, v, o, dout, lse):
        c, h, d = q.shape
        assert 2 * h == n and d == 2 * TB and c % (2 * TB) == 0 and n * TB % 128 == 0
        ni = c // (2 * TB)
        blk = n * TB
        chunk = 2 * TB * h
        f32, bf16 = jnp.float32, jnp.bfloat16
        flat = [a.reshape(c * h, d) for a in (q, dout, k, v)]
        dd = jnp.einsum('qhd,qhd->hq', dout, o, preferred_element_type=f32)
        vmem, dma = pltpu.VMEM, pltpu.SemaphoreType.DMA
        hbm = pl.BlockSpec(memory_space=pl.ANY)
        outs = pl.pallas_call(
            functools.partial(_kernel, n, h, d ** -0.5),
            out_shape=[jax.ShapeDtypeStruct((h, c, d), bf16)] * 3,
            in_specs=[hbm] * 4 + [pl.BlockSpec(memory_space=vmem)] * 2,
            out_specs=[hbm] * 3,
            scratch_shapes=[
                vmem((4, ni, chunk, d), bf16),
                vmem((2, 4, chunk, d), f32),
                vmem((4, h, c, d), bf16),
                vmem((h, ni, 2, 2 * TB), f32),
                vmem((2 * ni, n, TB, d), bf16),
                vmem((2 * ni, n, TB, d), bf16),
                vmem((ni, n, TB, d), bf16),
                vmem((ni, n, TB, d), bf16),
                vmem((ni, d, blk), bf16),
                vmem((n, ni, 2, 2 * TB), f32),
                vmem((ni, 2, 2 * blk), f32),
                vmem((blk, blk), jnp.int32),
                vmem((2 * ni, d, blk), f32),
                vmem((ni, d, blk), f32),
                vmem((ni, blk, d), f32),
                vmem((ni, blk, d), f32),
                vmem((ni, n, TB, d), bf16),
                vmem((ni, n, TB, d), bf16),
                vmem((ni, n, TB, d), bf16),
                vmem((3, h, c, d), bf16),
                dma((4, ni)), dma((5,)), dma((ni, 5)), dma((2,)), dma((ni, 2)), dma, dma((ni,)),
                dma((3,)), dma((3, ni)), dma((3, ni)),
            ],
            compiler_params=pltpu.CompilerParams(collective_id=0, has_side_effects=True,
                                                 vmem_limit_bytes=60 * 2 ** 20),
            name='attention_grads',
        )(*flat, lse, dd)
        steps = 4
        outs = pl.pallas_call(
            functools.partial(_merge_kernel, h, steps),
            out_shape=[jax.ShapeDtypeStruct((c * h, d), bf16)] * 3,
            in_specs=[hbm] * 3,
            out_specs=[hbm] * 3,
            scratch_shapes=[vmem((3, h, c, d), bf16), vmem((3, c * h, d), bf16), vmem((2, c // steps * h, d), f32),
                            dma((3, steps)), dma((3, steps))],
            compiler_params=pltpu.CompilerParams(vmem_limit_bytes=60 * 2 ** 20),
            name='merge_heads',
        )(*outs)
        return tuple(a.reshape(c, h, d) for a in outs)

    return jax.shard_map(local, mesh=mesh, in_specs=(rows, rows, rows, rows, rows, cols),
                         out_specs=(rows, rows, rows), check_vma=False)
```
